32 devices in a mesh: group: 8 (over z, y), local: 4 (over x, core).
Axes of the slice: x: 2, y: 2, z: 4, core: 2. Of those that a mesh axis runs over, the one named last changes fastest.
Arguments:
- dense_vec: bfloat16 [4096, 128], P(('group', 'local')), may hold values from -6 to 6
- q_tables: float32 [1024, 26, 128], P('group'), may hold values from -4 to 4
- r_tables: float32 [256, 26, 128], P('local'), may hold values from -4 to 4
- owner: int32 [4096, 26, 1], P(('group', 'local')), may hold values from 0 to 7; in each aligned block of 3328 rows (0 to 3327, 3328 to 6655, ..., all dimensions but the last counted through in order) at most 832 rows name the same one
- q_local: int32 [4096, 26], P(('group', 'local')), may hold values from 0 to 127
- r_index: int32 [4096, 26], P(('group', 'local')), may hold values from 0 to 255
- w_one: bfloat16 [479, 1024], replicated, may hold values from -0.25 to 0.25
- b_one: float32 [1024], replicated, may hold values from -3 to 3
- w_two: bfloat16 [1024, 1024], replicated, may hold values from -0.1875 to 0.1875
- b_two: float32 [1024], replicated, may hold values from -3 to 3
- w_three: bfloat16 [1024, 512], replicated, may hold values from -0.1875 to 0.1875
- b_three: float32 [512], replicated, may hold values from -3 to 3
- w_four: bfloat16 [512, 256], replicated, may hold values from -0.25 to 0.25
- b_four: float32 [256], replicated, may hold values from -3 to 3
- cotangent: bfloat16 [4096, 256], P(('group', 'local')), may hold values from -6 to 6
Outputs:
- q_new: float32 [1024, 26, 128], P('group')
- r_new: float32 [256, 26, 128], P('local')
- w_one_new: float32 [479, 1024], replicated
- b_one_new: float32 [1024], replicated
- w_two_new: float32 [1024, 1024], replicated
- b_two_new: float32 [1024], replicated
- w_three_new: float32 [1024, 512], replicated
- b_three_new: float32 [512], replicated
- w_four_new: float32 [512, 256], replicated
- b_four_new: float32 [256], replicated
The draws below stay inside these ranges and needn't reach their ends.
Inputs may be any that keep to these rules, and one draw needn't show every extreme that they name: `owner`: within the rows of one device (its 128 samples times 26 tables), no group is named more than 832 times, a bound that some block reaches.
All inputs are finite; a program needn't handle non-finite values.
Results may differ from the reference program's by a relative error of at most 0.0025.
Values may be sent and summed in bfloat16 or wider, within the bound.
A program may use at most 128 MiB of HBM per device.

```python
import math
import jax
import jax.numpy as jnp
import numpy as np
from jax import lax

TABLES = 26
DIM = 128
H1 = 1024
H2 = 1024
H3 = 512
H4 = 256
B_DEV = 128
QUOT_DEV = 128
FEAT = 479
BATCH = 4096
QUOT_ROWS = 1024
REM_ROWS = 256
CAP = 832
N_GROUP = 8
N_LOCAL = 4


def plant(result, own_key, least, largest):
    index_at = [jax.random.randint(jax.random.fold_in(own_key, axis), (), 0, length) for axis, length in enumerate(result.shape)]
    longest = result.shape.index(max(result.shape))
    beside = index_at[:longest] + [(index_at[longest] + 1) % result.shape[longest]] + index_at[longest + 1:]
    return result.at[tuple(index_at)].set(least).at[tuple(beside)].set(largest)


def levels(rng, extent, pieces, low, top_value):
    gain, own = 1.0, jax.random.fold_in(rng, 6)
    for position, parts in pieces:
        steps = jnp.exp(jax.random.uniform(jax.random.fold_in(own, position), (parts,), jnp.float32, low / len(pieces), top_value / len(pieces)))
        gain = gain * jnp.repeat(steps, extent[position] // parts).reshape([-1 if axis == position else 1 for axis in range(len(extent))])
    return gain


def rank_bounds(number_of, skew):
    loads = [(1 << 20) // math.isqrt(standing ** skew) + 1 for standing in range(1, number_of + 1)]
    deviation = 1 + sum(loads) // (1 << 30)
    return np.cumsum(np.array([max(1, weight // deviation) for weight in loads]))


def skewed_ids(own_key, dims, count, lean):
    listing = rank_bounds(count, lean)
    pick = jax.random.randint(jax.random.fold_in(own_key, 1), dims, 0, int(listing[count - 1]))
    grade = jnp.searchsorted(jnp.asarray(listing, jnp.int32), pick, side="right")
    return jax.random.permutation(jax.random.fold_in(own_key, 2), count)[grade].astype(jnp.int32)


def routed_block(stream_key, own, number, rows, amount, top, limit, lean):
    ranking = jax.random.permutation(stream_key, amount)
    packed, usual = portions_of(amount, rows * top, limit, lean, True), portions_of(amount, rows * top, limit, lean, False)
    places = jnp.arange(amount)

    def named(tallies, rotation):
        used = int((tallies > 0).sum())
        fixed = max(1, used // 4)
        passed = fixed + (places - fixed + rotation * (used - fixed)) % max(1, amount - fixed)
        return jnp.zeros((amount,), jnp.int32).at[ranking[jnp.where(places < fixed, places, passed)]].set(jnp.asarray(tallies, jnp.int32))

    tallies = jnp.where(number % 4 == 0, named(packed, number // 4), named(usual, number - number // 4 - 1))
    mixed = jax.random.permutation(jax.random.fold_in(own, 3), amount)
    source_of, receiver = mixed[0:amount // 2 * 2:2], mixed[1:amount // 2 * 2:2]
    slack = jnp.minimum(tallies[source_of] - 1, limit - tallies[receiver]) // 2
    slack = jnp.where((source_of == ranking[0]) | (receiver == ranking[0]) | (tallies[receiver] == 0), 0, jnp.maximum(slack, 0))
    passed = jax.random.randint(jax.random.fold_in(own, 4), (amount // 2,), 0, 1 << 20) % (slack + 1)
    tallies = tallies.at[source_of].add(-passed).at[receiver].add(passed)
    items = jnp.searchsorted(jnp.cumsum(tallies), jnp.arange(rows * top), side="right").astype(jnp.int32)
    table = items.reshape(top, rows).T
    table = table[jax.random.permutation(jax.random.fold_in(own, 1), rows)]
    rotation = jax.random.randint(jax.random.fold_in(own, 2), (rows, 1), 0, top)
    return jnp.take_along_axis(table, (jnp.arange(top)[None, :] + rotation) % top, axis=1)


def portions_of(number_of, total, reach, slope, full):
    loads = [(1 << 20) // math.isqrt(rank ** slope) + 1 for rank in range(1, number_of + 1)]
    largest = reach if full else min(reach, max(-(-total // number_of), total * loads[0] // sum(loads)))
    least = 1 if total - largest >= number_of - 1 else 0
    holding, surplus = [largest] + [least] * (number_of - 1), total - largest - least * (number_of - 1)
    while surplus > 0:
        free = [i for i in range(1, number_of) if holding[i] < largest] or [i for i in range(1, number_of) if holding[i] < reach]
        whole, left = sum([loads[i] for i in free]), surplus
        for i in free:
            more = min(reach - holding[i], max(1, left * loads[i] // whole), surplus)
            holding[i] = holding[i] + more
            surplus = surplus - more
    return np.array(holding)


def centred(stream_key, extent, scale, reach, pieces=(), held_as=jnp.bfloat16):
    factor_of = levels(stream_key, extent, pieces, -0.22, 0.18) if pieces else 1.0
    result = jax.random.normal(stream_key, extent, jnp.float32) * scale * factor_of
    return jnp.minimum(jnp.maximum(result, -reach), reach).astype(held_as)


def setup_inputs(seed: int = 0) -> dict:
    streams_of = jax.random.split(jax.random.key(seed), 16)
    dense_vec = centred(streams_of[0], (BATCH, DIM), 1.0, 6.0, ((0, 32),))
    q_tables = centred(streams_of[1], (QUOT_ROWS, TABLES, DIM), 0.5, 4.0, ((0, 8),), jnp.float32)
    r_tables = centred(streams_of[2], (REM_ROWS, TABLES, DIM), 0.5, 4.0, ((0, 4),), jnp.float32)
    owner_keys = jax.random.split(jax.random.fold_in(streams_of[3], 1), BATCH * TABLES // (B_DEV * TABLES))
    owner_turns = jax.random.permutation(jax.random.fold_in(streams_of[3], 3), BATCH * TABLES // (B_DEV * TABLES))
    owner = jax.vmap(lambda own, number: routed_block(jax.random.fold_in(streams_of[3], 2), own, number, B_DEV * TABLES, N_GROUP, 1, CAP, 2))(owner_keys, owner_turns).reshape((BATCH, TABLES, 1))
    q_local = plant(skewed_ids(streams_of[4], (BATCH, TABLES), QUOT_DEV, 2), jax.random.fold_in(streams_of[4], 3), 0, QUOT_DEV - 1).astype(jnp.int32)
    r_index = plant(jax.random.randint(streams_of[5], (BATCH, TABLES), 0, REM_ROWS), jax.random.fold_in(streams_of[5], 1), 0, REM_ROWS - 1).astype(jnp.int32)
    w_one = centred(streams_of[6], (FEAT, H1), FEAT ** -0.5, 0.25)
    b_one = centred(streams_of[7], (H1,), 0.5, 3.0, (), jnp.float32)
    w_two = centred(streams_of[8], (H1, H2), H1 ** -0.5, 0.1875)
    b_two = centred(streams_of[9], (H2,), 0.5, 3.0, (), jnp.float32)
    w_three = centred(streams_of[10], (H2, H3), H2 ** -0.5, 0.1875)
    b_three = centred(streams_of[11], (H3,), 0.5, 3.0, (), jnp.float32)
    w_four = centred(streams_of[12], (H3, H4), H3 ** -0.5, 0.25)
    b_four = centred(streams_of[13], (H4,), 0.5, 3.0, (), jnp.float32)
    cotangent = centred(streams_of[14], (BATCH, H4), 1.0, 6.0, ((0, 32),))
    return dict(dense_vec=dense_vec, q_tables=q_tables, r_tables=r_tables, owner=owner, q_local=q_local, r_index=r_index, w_one=w_one, b_one=b_one, w_two=w_two, b_two=b_two, w_three=w_three, b_three=b_three, w_four=w_four, b_four=b_four, cotangent=cotangent)


table_rate = 0.05
dense_rate = 0.0005


def silu_slope(preact):
    sigma = jax.nn.sigmoid(preact)
    return sigma * (1.0 + preact * (1.0 - sigma))


def interact(dense_rows, embeds):
    vectors_all = jnp.concatenate([dense_rows[:, None, :], embeds], axis=1).astype(jnp.float32)
    gram_mat = jnp.einsum("bid,bjd->bij", vectors_all, vectors_all, precision=lax.Precision.HIGHEST)
    lower_i, lower_j = np.tril_indices(vectors_all.shape[1], -1)
    pair_vals = gram_mat[:, lower_i, lower_j]
    features = jnp.concatenate([dense_rows.astype(jnp.float32), pair_vals], axis=1).astype(jnp.bfloat16)
    return vectors_all, features


def pair_back(d_pairs, vectors_all):
    vectors = vectors_all.shape[1]
    lower_i, lower_j = np.tril_indices(vectors, -1)
    spread = jnp.zeros((vectors_all.shape[0], vectors, vectors), jnp.float32).at[:, lower_i, lower_j].set(d_pairs)
    spread = spread + jnp.swapaxes(spread, 1, 2)
    return jnp.einsum("bij,bjd->bid", spread, vectors_all, precision=lax.Precision.HIGHEST)


def contract_rows(left, right):
    return lax.dot_general(left, right, (((0,), (0,)), ((), ())), preferred_element_type=jnp.float32)


def dense_pass(features, layers, cot_rows):
    inputs_list = [features]
    pre_list = []
    current = features
    for layer_idx, (weight, biases) in enumerate(layers):
        pre_act = jnp.dot(current, weight, preferred_element_type=jnp.float32) + biases
        pre_list.append(pre_act)
        if layer_idx + 1 < len(layers):
            current = jax.nn.silu(pre_act).astype(jnp.bfloat16)
            inputs_list.append(current)
    grad_low = cot_rows
    grad_full = cot_rows.astype(jnp.float32)
    grads = []
    back_grad = None
    for layer_idx in reversed(range(len(layers))):
        weight = layers[layer_idx][0]
        w_grad = contract_rows(inputs_list[layer_idx], grad_low)
        b_grad = jnp.sum(grad_full, axis=0)
        back_grad = lax.dot_general(grad_low, weight, (((1,), (1,)), ((), ())), preferred_element_type=jnp.float32)
        grads.insert(0, (w_grad, b_grad))
        if layer_idx > 0:
            grad_full = back_grad * silu_slope(pre_list[layer_idx - 1])
            grad_low = grad_full.astype(jnp.bfloat16)
    return grads, back_grad


def reference(dense_vec, q_tables, r_tables, owner, q_local, r_index, w_one, b_one, w_two, b_two, w_three, b_three, w_four, b_four, cotangent):
    layers = [(w_one, b_one), (w_two, b_two), (w_three, b_three), (w_four, b_four)]
    block = B_DEV * N_LOCAL
    block_count = BATCH // block
    table_ids = jnp.arange(TABLES, dtype=jnp.int32)[None, :]
    q_flat_table = q_tables.reshape(QUOT_ROWS * TABLES, DIM)
    r_flat_table = r_tables.reshape(REM_ROWS * TABLES, DIM)
    owner_all = owner[:, :, 0]

    def block_step(totals, offset):
        q_grad, r_grad, dense_grads = totals
        dense_rows = lax.dynamic_slice_in_dim(dense_vec, offset, block, 0)
        owner_rows = lax.dynamic_slice_in_dim(owner_all, offset, block, 0)
        local_rows = lax.dynamic_slice_in_dim(q_local, offset, block, 0)
        rem_rows = lax.dynamic_slice_in_dim(r_index, offset, block, 0)
        cot_rows = lax.dynamic_slice_in_dim(cotangent, offset, block, 0)
        q_flat = ((owner_rows * QUOT_DEV + local_rows) * TABLES + table_ids).reshape(-1).astype(jnp.int32)
        r_flat = (rem_rows * TABLES + table_ids).reshape(-1).astype(jnp.int32)
        q_rows = q_flat_table[q_flat].astype(jnp.bfloat16)
        r_rows = r_flat_table[r_flat]
        q_val = q_rows.astype(jnp.float32)
        embeds = (q_val * r_rows).astype(jnp.bfloat16).reshape(block, TABLES, DIM)
        vectors_all, features = interact(dense_rows, embeds)
        grads, d_features = dense_pass(features, layers, cot_rows)
        d_embed = pair_back(d_features[:, DIM:], vectors_all)[:, 1:, :].reshape(-1, DIM)
        q_grad = q_grad.at[q_flat].add(d_embed * r_rows)
        r_grad = r_grad.at[r_flat].add(d_embed * q_val)
        dense_grads = jax.tree.map(jnp.add, dense_grads, grads)
        return (q_grad, r_grad, dense_grads), None

    start_grads = [(jnp.zeros(weight.shape, jnp.float32), jnp.zeros(biases.shape, jnp.float32)) for weight, biases in layers]
    start_totals = (jnp.zeros((QUOT_ROWS * TABLES, DIM), jnp.float32), jnp.zeros((REM_ROWS * TABLES, DIM), jnp.float32), start_grads)
    offsets = jnp.arange(block_count, dtype=jnp.int32) * block
    (q_grad, r_grad, dense_grads), unused = lax.scan(block_step, start_totals, offsets)
    q_new = q_tables - table_rate * q_grad.reshape(q_tables.shape)
    r_new = r_tables - table_rate * r_grad.reshape(r_tables.shape)
    updated = []
    for (weight, biases), (w_grad, b_grad) in zip(layers, dense_grads):
        updated.append(weight.astype(jnp.float32) - dense_rate * w_grad)
        updated.append(biases - dense_rate * b_grad)
    return (q_new, r_new, updated[0], updated[1], updated[2], updated[3], updated[4], updated[5], updated[6], updated[7])
```

```python
import functools

import jax
import jax.numpy as jnp
from jax import lax
from jax.experimental import pallas as pl
from jax.experimental.pallas import tpu as pltpu
from jax.sharding import PartitionSpec as P

table_rate = 0.05
dense_rate = 0.0005
F32 = jnp.float32
BF16 = jnp.bfloat16
HIGHEST = lax.Precision.HIGHEST


def silu_slope(preact):
    sigma = jax.nn.sigmoid(preact)
    return sigma * (1.0 + preact * (1.0 - sigma))


def contract_rows(left, right):
    return lax.dot_general(left, right, (((0,), (0,)), ((), ())), preferred_element_type=F32)


def index_row(pack_ref, row):
    return jnp.concatenate(
        [pack_ref[s, 0, pl.ds(row, 1), :] for s in range(pack_ref.shape[0])], axis=1
    )


def pick_matrix(index, count):
    rows = lax.broadcasted_iota(jnp.int32, (count, index.shape[1]), 0)
    return rows == index.astype(jnp.int32)


def lookup_kernel(q_ref, pack_ref, emb_ref, q_out, r_out):
    groups, _, q_rows, width = q_ref.shape
    locals_, _, pack_rows, batch = pack_ref.shape
    r_rows = pack_rows - 8
    q_table = q_ref[:, 0].reshape(groups * q_rows, width)
    r_table = pack_ref[:, 0, :r_rows, :].reshape(locals_ * r_rows, width)
    q_hit = pick_matrix(index_row(pack_ref, r_rows), groups * q_rows).astype(F32).astype(BF16)
    r_hit = pick_matrix(index_row(pack_ref, r_rows + 1), locals_ * r_rows).astype(F32)
    over_rows = (((0,), (0,)), ((), ()))
    q_val = lax.dot_general(q_table, q_hit, over_rows, preferred_element_type=F32)
    r_val = lax.dot_general(
        r_table, r_hit, over_rows, preferred_element_type=F32, precision=HIGHEST
    )
    q_out[0] = q_val.astype(BF16)
    r_out[0] = r_val
    embeds = (q_val * r_val).astype(BF16)
    for s in range(locals_):
        emb_ref[s, 0] = embeds[:, s * batch : (s + 1) * batch]


def table_grad_kernel(d_ref, pack_ref, q_ref, r_ref, qg_ref, rg_ref):
    locals_, _, pack_rows, batch = pack_ref.shape
    r_rows = pack_rows - 8
    groups, _, q_rows, width = qg_ref.shape
    d_embed = jnp.concatenate([d_ref[s, 0] for s in range(locals_)], axis=1).astype(F32)
    q_hit = pick_matrix(index_row(pack_ref, r_rows), groups * q_rows).astype(F32).astype(BF16)
    r_hit = pick_matrix(index_row(pack_ref, r_rows + 1), locals_ * r_rows).astype(F32)
    over_lanes = (((1,), (1,)), ((), ()))
    q_terms = (d_embed * r_ref[0]).astype(BF16)
    r_terms = d_embed * q_ref[0].astype(F32)
    q_grad = lax.dot_general(q_hit, q_terms, over_lanes, preferred_element_type=F32)
    r_grad = lax.dot_general(
        r_hit, r_terms, over_lanes, preferred_element_type=F32, precision=HIGHEST
    )
    qg_ref[:, 0] = q_grad.astype(BF16).reshape(groups, q_rows, width)
    rg_ref[:, 0] = r_grad.reshape(locals_, r_rows, width)


def load_vectors(dense_ref, emb_ref, vec_ref, tables):
    vec_ref[0] = dense_ref[...].astype(F32)

    def fill(t, carry):
        vec_ref[t + 1] = emb_ref[t].astype(F32)
        return carry

    lax.fori_loop(0, tables, fill, 0)
    for t in range(tables + 1, vec_ref.shape[0]):
        vec_ref[t] = jnp.zeros(vec_ref.shape[1:], F32)


def gram_kernel(tables, dense_ref, emb_ref, feat_ref, vec_ref, row_ref):
    width = dense_ref.shape[0]
    load_vectors(dense_ref, emb_ref, vec_ref, tables)

    def outer(i, carry):
        mine = vec_ref[i]
        base = (i * (i - 1)) >> 1

        def inner(k, inner_carry):
            for u in range(4):
                j = 4 * k + u
                row_ref[pl.ds(base + j, 1), :] = jnp.sum(mine * vec_ref[j], axis=0, keepdims=True)
            return inner_carry

        return lax.fori_loop(0, (i + 3) >> 2, inner, carry)

    lax.fori_loop(1, tables + 1, outer, 0)
    pairs = feat_ref.shape[0] - width
    feat_ref[:width, :] = dense_ref[...]
    feat_ref[width:, :] = row_ref[:pairs, :].astype(BF16)


def pair_kernel(tables, d_ref, dense_ref, emb_ref, out_ref, vec_ref):
    width = dense_ref.shape[0]
    pairs = d_ref.shape[0] - width
    load_vectors(dense_ref, emb_ref, vec_ref, tables)

    def outer(i, carry):
        total = jnp.zeros(vec_ref.shape[1:], F32)
        for j in range(tables + 1):
            below = ((i * (i - 1)) >> 1) + j
            above = (j * (j - 1)) // 2 + i
            place = jnp.minimum(jnp.where(j < i, below, above), pairs - 1)
            row = d_ref[pl.ds(width + place, 1), :]
            row = jnp.where(i == j, jnp.zeros_like(row), row)
            total = total + row * vec_ref[j]
        out_ref[i - 1] = total.astype(BF16)
        return carry

    lax.fori_loop(1, tables + 1, outer, 0)
    for t in range(tables, out_ref.shape[0]):
        out_ref[t] = jnp.zeros(out_ref.shape[1:], BF16)


def whole(count):
    return [pl.BlockSpec(memory_space=pltpu.VMEM)] * count


def body(
    dense_vec,
    q_tables,
    r_tables,
    owner,
    q_local,
    r_index,
    w_one,
    b_one,
    w_two,
    b_two,
    w_three,
    b_three,
    w_four,
    b_four,
    cotangent,
):
    weights = [w_one, w_two, w_three, w_four]
    biases = [b_one, b_two, b_three, b_four]
    groups = lax.axis_size("group")
    locals_ = lax.axis_size("local")
    here = lax.axis_index("local")
    batch, tables = q_local.shape
    q_rows, _, width = q_tables.shape
    r_rows = r_tables.shape[0]
    share = -(-tables // locals_)
    padded = share * locals_
    extra = padded - tables

    q_major = jnp.transpose(jnp.pad(q_tables, ((0, 0), (0, extra), (0, 0))), (1, 0, 2))
    q_mine = lax.dynamic_slice_in_dim(q_major, here * share, share, 0)
    q_all = lax.all_gather(q_mine.astype(BF16), "group", axis=0, tiled=False)
    r_major = jnp.transpose(jnp.pad(r_tables, ((0, 0), (0, extra), (0, 0))), (1, 0, 2))
    q_index = (owner[:, :, 0] * q_rows + q_local).astype(F32)
    indices = jnp.stack([q_index, r_index.astype(F32)], axis=0)
    indices = jnp.transpose(jnp.pad(indices, ((0, 6), (0, 0), (0, extra))), (2, 0, 1))
    pack = jnp.concatenate([r_major, indices], axis=1)
    pack = pack.reshape(locals_, share, r_rows + 8, width)
    pack = lax.all_to_all(pack, "local", split_axis=0, concat_axis=0, tiled=True)

    def spec(lead, *tail):
        return pl.BlockSpec((lead, 1) + tail, lambda t: (0, t) + (0,) * len(tail))

    def flat(*tail):
        return pl.BlockSpec((1,) + tail, lambda t: (t,) + (0,) * len(tail))

    many = locals_ * batch
    work = 2 * share * many * width * (groups * q_rows + 6 * locals_ * r_rows)
    cost = pl.CostEstimate(flops=work, bytes_accessed=8 << 20, transcendentals=0)
    embeds, q_val, r_val = pl.pallas_call(
        lookup_kernel,
        grid=(share,),
        in_specs=[spec(groups, q_rows, width), spec(locals_, r_rows + 8, width)],
        out_specs=[spec(locals_, width, batch), flat(width, many), flat(width, many)],
        out_shape=[
            jax.ShapeDtypeStruct((locals_, share, width, batch), BF16),
            jax.ShapeDtypeStruct((share, width, many), BF16),
            jax.ShapeDtypeStruct((share, width, many), F32),
        ],
        cost_estimate=cost,
        name="lookup",
    )(q_all, pack)
    embeds = lax.all_to_all(embeds, "local", split_axis=0, concat_axis=0, tiled=True)
    embeds = embeds.reshape(padded, width, batch)

    dense_t = dense_vec.T
    steps = 4 * (-(-tables // 4))
    slots = max(steps, tables + 1)
    pairs = tables * (tables + 1) // 2
    row_slots = -(-(tables * (tables - 1) // 2 + steps) // 8) * 8
    vec_scratch = pltpu.VMEM((slots, width, batch), F32)
    pair_cost = pl.CostEstimate(
        flops=64 * pairs * width * batch, bytes_accessed=2 << 20, transcendentals=0
    )
    features_t = pl.pallas_call(
        functools.partial(gram_kernel, tables),
        in_specs=whole(2),
        out_specs=whole(1)[0],
        out_shape=jax.ShapeDtypeStruct((width + pairs, batch), BF16),
        scratch_shapes=[vec_scratch, pltpu.VMEM((row_slots, batch), F32)],
        cost_estimate=pair_cost,
        name="gram",
    )(dense_t, embeds)

    inputs = [None]
    pres = []
    current = None
    for k in range(4):
        if k == 0:
            pre = contract_rows(features_t, weights[0]) + biases[0]
        else:
            pre = jnp.dot(current, weights[k], preferred_element_type=F32) + biases[k]
        pres.append(pre)
        if k < 3:
            current = jax.nn.silu(pre).astype(BF16)
            inputs.append(current)
    grad_low = cotangent
    grad_full = cotangent.astype(F32)
    w_grads, b_grads = [None] * 4, [None] * 4
    for k in (3, 2, 1, 0):
        b_grads[k] = jnp.sum(grad_full, axis=0)
        if k:
            w_grads[k] = contract_rows(inputs[k], grad_low)
            back = lax.dot_general(
                grad_low, weights[k], (((1,), (1,)), ((), ())), preferred_element_type=F32
            )
            grad_full = back * silu_slope(pres[k - 1])
            grad_low = grad_full.astype(BF16)
        else:
            w_grads[0] = jnp.dot(features_t, grad_low, preferred_element_type=F32)
    d_features_t = lax.dot_general(
        w_one, grad_low, (((1,), (1,)), ((), ())), preferred_element_type=F32
    )

    d_embeds = pl.pallas_call(
        functools.partial(pair_kernel, tables),
        in_specs=whole(3),
        out_specs=whole(1)[0],
        out_shape=jax.ShapeDtypeStruct((padded, width, batch), BF16),
        scratch_shapes=[vec_scratch],
        cost_estimate=pair_cost,
        name="pair_back",
    )(d_features_t, dense_t, embeds)
    d_embeds = lax.all_to_all(
        d_embeds.reshape(locals_, share, width, batch),
        "local",
        split_axis=0,
        concat_axis=0,
        tiled=True,
    )
    q_part, r_part = pl.pallas_call(
        table_grad_kernel,
        grid=(share,),
        in_specs=[
            spec(locals_, width, batch),
            spec(locals_, r_rows + 8, width),
            flat(width, many),
            flat(width, many),
        ],
        out_specs=[spec(groups, q_rows, width), spec(locals_, r_rows, width)],
        out_shape=[
            jax.ShapeDtypeStruct((groups, share, q_rows, width), BF16),
            jax.ShapeDtypeStruct((locals_, share, r_rows, width), F32),
        ],
        cost_estimate=cost,
        name="table_grad",
    )(d_embeds, pack, q_val, r_val)

    q_piece = lax.psum_scatter(q_part, "group", scatter_dimension=0, tiled=False).astype(F32)
    q_mine_new = lax.all_gather(q_mine - table_rate * q_piece, "local", axis=0, tiled=False)
    q_new = jnp.transpose(q_mine_new.reshape(padded, q_rows, width)[:tables], (1, 0, 2))

    bias_sizes = [b.shape[0] for b in biases]
    bias_total = sum(bias_sizes)
    bias_rows = -(-bias_total // (8 * width)) * 8
    b_flat = jnp.concatenate(b_grads + [jnp.zeros((bias_rows * width - bias_total,), F32)])
    b_block = jnp.broadcast_to(
        b_flat.reshape(1, bias_rows, width), (locals_, bias_rows, width)
    )
    mixed = jnp.concatenate([r_part.reshape(locals_, share * r_rows, width), b_block], axis=1)
    mixed = lax.all_to_all(mixed, "local", split_axis=0, concat_axis=0, tiled=True)
    r_lines = mixed[:, : share * r_rows, :].reshape(padded * r_rows, width)
    b_lines = jnp.sum(mixed[:, share * r_rows :, :], axis=0)
    summed = lax.psum(jnp.concatenate([r_lines, b_lines], axis=0), "group")
    r_grad = summed[: tables * r_rows].reshape(tables, r_rows, width)
    r_new = r_tables - table_rate * jnp.transpose(r_grad, (1, 0, 2))
    b_sum = summed[padded * r_rows :].reshape(-1)

    w_sums = lax.psum([g.astype(BF16) for g in w_grads], ("group", "local"))
    updated = []
    start = 0
    for weight, bias, w_sum, size in zip(weights, biases, w_sums, bias_sizes):
        updated.append(weight.astype(F32) - dense_rate * w_sum.astype(F32))
        updated.append(bias - dense_rate * b_sum[start : start + size])
        start += size
    return (q_new, r_new) + tuple(updated)


def solution(mesh):
    rows = P(("group", "local"), None)
    return jax.shard_map(
        body,
        mesh=mesh,
        in_specs=(
            rows,
            P("group", None, None),
            P("local", None, None),
            P(("group", "local"), None, None),
            rows,
            rows,
            P(),
            P(),
            P(),
            P(),
            P(),
            P(),
            P(),
            P(),
            rows,
        ),
        out_specs=(P("group", None, None), P("local", None, None)) + (P(),) * 8,
        check_vma=False,
    )
```
